256 devices in a mesh: section: 8 (over y_hi, x), tensor: 16 (over z, core), dp: 2 (over y_lo).
Axes of the slice: x: 4, y: 4 (y_hi: 2, y_lo: 2; y = y_hi * 2 + y_lo), z: 8, core: 2. Of those that a mesh axis runs over, the one named last changes fastest.
Arguments:
- dec_queries: bfloat16 [8, 4, 512, 16384], P('section', 'dp', None, 'tensor'), may hold values from -8 to 8
- enc_keys: bfloat16 [8, 4, 512, 16384], P('section', 'dp', None, 'tensor'), may hold values from -4 to 4
- enc_values: bfloat16 [8, 4, 512, 16384], P('section', 'dp', None, 'tensor'), may hold values from -4 to 4
- out_grad: bfloat16 [8, 4, 512, 16384], P('section', 'dp', None, 'tensor'), may hold values from -15 to 15
- key_weight: bfloat16 [8, 1024, 16384], P('section', None, 'tensor'), may hold values from -0.1875 to 0.1875
- value_weight: bfloat16 [8, 1024, 16384], P('section', None, 'tensor'), may hold values from -0.1875 to 0.1875
- enc_hidden: float32 [4, 512, 1024], P('dp', 'section', 'tensor'), may hold values from -2 to 2, as said below
- enc_gain: float32 [1024], P('tensor'), may hold values from 0.1 to 1.9
Outputs:
- enc_input_grad: float32 [4, 512, 1024], P('dp', 'section', 'tensor')
The draws below stay inside these ranges and needn't reach their ends.
Inputs may be any that keep to these rules, and one draw needn't show every extreme that they name: `enc_hidden`: every entry's magnitude is at least 0.25.
All inputs are finite; a program needn't handle non-finite values.
Results may differ from the reference program's by a relative error of at most 0.0041.
Values sent between devices are 32-bit elements; how exact they have to be, the bound alone decides.
No kernel may reach another device: no remote copies, remote signals or barrier semaphores. Data moves between devices by JAX's collectives and lax.ppermute only.
A program may use at most 128 MiB of HBM per device.

```python
import jax
import jax.numpy as jnp
from jax import lax

D = 1024
DK = 128
DEC = 512
ENC = 512
HEADS = 128
INNER = 16384
SECTIONS = 8
SEQS = 4


def shared_rows(key):
    return jnp.clip(jax.random.normal(jax.random.fold_in(key, 12), (SECTIONS, SEQS, 1, INNER), jnp.float32), -4.0, 4.0)


def aligned_spot(key):
    return jax.random.randint(jax.random.fold_in(key, 13), (), 0, ENC).astype(jnp.int32)


def draw_enc_keys(key, part):
    base = jnp.clip(jax.random.normal(jax.random.fold_in(key, 11), (SECTIONS, SEQS, ENC, INNER), jnp.float32), -4.0, 4.0)
    zero = jnp.zeros((), jnp.int32)
    base = lax.dynamic_update_slice(base, shared_rows(key), (zero, zero, aligned_spot(key), zero))
    return base.astype(jnp.bfloat16)


def draw_dec_queries(key, part):
    base = 0.1 * jnp.clip(jax.random.normal(jax.random.fold_in(key, 22), (SECTIONS, SEQS, DEC, INNER), jnp.float32), -6.0, 6.0)
    return base.astype(jnp.bfloat16)


def draw_enc_hidden(key, part):
    shape = (SEQS, ENC, D)
    own_sign = jnp.where(jax.random.bernoulli(jax.random.fold_in(key, 31), 0.5, shape), 1.0, -1.0)
    magnitude = jax.random.uniform(jax.random.fold_in(key, 36), shape, jnp.float32, 0.25, 2.0)
    sign = own_sign
    return (sign * magnitude).astype(jnp.float32)


def levels(key, dims, cuts, smallest, high):
    factor_of, own = 1.0, jax.random.fold_in(key, 6)
    for position, parts in cuts:
        draws = jnp.exp(jax.random.uniform(jax.random.fold_in(own, position), (parts,), jnp.float32, smallest / len(cuts), high / len(cuts)))
        factor_of = factor_of * jnp.repeat(draws, dims[position] // parts).reshape([-1 if axis == position else 1 for axis in range(len(dims))])
    return factor_of


def normal_values(rng, extent, spread, most, shards=(), kind=jnp.bfloat16):
    values = jax.random.normal(rng, extent, jnp.float32) * spread
    if len(shards) > 0:
        values = levels(rng, extent, shards, -0.22, 0.18) * values
    return jnp.clip(values, min=-most, max=most).astype(kind)


def setup_inputs(seed: int = 0) -> dict:
    seeds = jax.random.split(jax.random.key(seed), 9)
    return {
        "dec_queries": draw_dec_queries(jax.random.fold_in(seeds[8], 71), 0),
        "enc_keys": draw_enc_keys(jax.random.fold_in(seeds[8], 71), 0),
        "enc_values": normal_values(seeds[2], (SECTIONS, SEQS, ENC, INNER), 1.0, 4.0, ((0, 8), (1, 2), (3, 16))),
        "out_grad": normal_values(seeds[3], (SECTIONS, SEQS, DEC, INNER), 3.0, 15.0, ((0, 8), (1, 2), (3, 16))),
        "key_weight": normal_values(seeds[4], (SECTIONS, D, INNER), D ** -0.5, 0.1875, ((0, 8), (2, 16))),
        "value_weight": normal_values(seeds[5], (SECTIONS, D, INNER), D ** -0.5, 0.1875, ((0, 8), (2, 16))),
        "enc_hidden": draw_enc_hidden(jax.random.fold_in(seeds[8], 71), 0),
        "enc_gain": jnp.clip(1.0 + 0.18 * jax.random.normal(seeds[7], (D,), jnp.float32), 0.1, 1.9),
    }


def attention_grads(query, keyset, valueset, gradset):
    query_heads = query.reshape(DEC, HEADS, DK).astype(jnp.float32)
    key_heads = keyset.reshape(ENC, HEADS, DK).astype(jnp.float32)
    value_heads = valueset.reshape(ENC, HEADS, DK).astype(jnp.float32)
    grad_heads = gradset.reshape(DEC, HEADS, DK).astype(jnp.float32)
    scores = jnp.einsum('qhd,khd->hqk', query_heads, key_heads)
    shifted = jnp.exp(scores - lax.optimization_barrier(jnp.max(scores, axis=-1, keepdims=True)))
    attn_probs = shifted / lax.optimization_barrier(jnp.sum(shifted, axis=-1, keepdims=True))
    probs_low = lax.optimization_barrier(attn_probs.astype(jnp.bfloat16)).astype(jnp.float32)
    attended = jnp.einsum('hqk,khd->qhd', probs_low, value_heads)
    row_dot = lax.optimization_barrier(jnp.sum(grad_heads * attended, axis=-1))
    value_grad = jnp.einsum('hqk,qhd->khd', probs_low, grad_heads).astype(jnp.bfloat16)
    prob_grad = jnp.einsum('qhd,khd->hqk', grad_heads, value_heads)
    score_grad = attn_probs * (prob_grad - jnp.transpose(row_dot)[:, :, None])
    score_low = lax.optimization_barrier(score_grad.astype(jnp.bfloat16)).astype(jnp.float32)
    key_grad = jnp.einsum('hqk,qhd->khd', score_low, query_heads).astype(jnp.bfloat16)
    return (key_grad.reshape(ENC, HEADS * DK), value_grad.reshape(ENC, HEADS * DK))

def reference(dec_queries, enc_keys, enc_values, out_grad, key_weight, value_weight, enc_hidden, enc_gain):

    def section_term(pieces):
        query, keyset, valueset, gradset, weight_k, weight_v = pieces

        def seq_term(inner):
            key_grad, value_grad = attention_grads(inner[0], inner[1], inner[2], inner[3])
            first = jnp.dot(key_grad, jnp.transpose(weight_k), preferred_element_type=jnp.float32)
            second = jnp.dot(value_grad, jnp.transpose(weight_v), preferred_element_type=jnp.float32)
            return first + second
        return lax.map(seq_term, (query, keyset, valueset, gradset))
    terms = lax.map(section_term, (dec_queries, enc_keys, enc_values, out_grad, key_weight, value_weight))
    enc_grad = lax.optimization_barrier(jnp.sum(terms, axis=0))
    scaled = enc_gain * enc_grad
    square_total = lax.optimization_barrier(jnp.sum(enc_hidden * enc_hidden, axis=-1))
    cross_total = lax.optimization_barrier(jnp.sum(scaled * enc_hidden, axis=-1))
    inverse = lax.rsqrt(square_total / D + 1e-06)
    return scaled * inverse[..., None] - enc_hidden * (cross_total * inverse * inverse * inverse / D)[..., None]
```

```python
import functools

import jax
import jax.numpy as jnp
from jax import lax
from jax.experimental import pallas as pl
from jax.experimental.pallas import tpu as pltpu
from jax.sharding import Mesh, PartitionSpec as P

D = 1024
DK = 128
epsilon = 1e-06
F32 = jnp.float32
BF16 = jnp.bfloat16
VMEM = pl.BlockSpec(memory_space=pltpu.VMEM)
SMEM = pl.BlockSpec(memory_space=pltpu.SMEM)
NT = (((1,), (1,)), ((), ()))
NN = (((1,), (0,)), ((), ()))
GIB = 2**20


def dot(a, b, dims):
    return lax.dot_general(a, b, dims, preferred_element_type=F32)


def by_owner(rows):
    return rows.reshape(2, 4, 64, DK).swapaxes(0, 1).reshape(512, DK)


def attention_kernel(heads, q_ref, k_ref, v_ref, g_ref, kg_ref, vg_ref):
    for h in range(heads):
        cols = pl.ds(h * DK, DK)
        k = by_owner(k_ref[0, 0, :, cols])
        v = by_owner(v_ref[0, 0, :, cols])
        kg, vg = None, None
        for part in range(2):
            rows = pl.ds(part * 256, 256)
            q = q_ref[0, 0, rows, cols]
            g = g_ref[0, 0, rows, cols]
            scores = dot(k, q, NT)
            shifted = jnp.exp(scores - jnp.max(scores, axis=0, keepdims=True))
            probs = shifted * (1.0 / jnp.sum(shifted, axis=0, keepdims=True))
            low = probs.astype(BF16)
            prob_grad = dot(v, g, NT)
            row_dot = jnp.sum(probs * prob_grad, axis=0, keepdims=True)
            score_low = (probs * (prob_grad - row_dot)).astype(BF16)
            vg_part = dot(low, g, NN)
            kg_part = dot(score_low, q, NN)
            vg = vg_part if vg is None else vg + vg_part
            kg = kg_part if kg is None else kg + kg_part
        kg_ref[:, cols] = kg.astype(BF16)
        vg_ref[:, cols] = vg.astype(BF16)


def attention(seq, q, k, v, g, heads=2):
    hidden = q.shape[3]
    steps = hidden // (heads * DK)
    spec = pl.BlockSpec((1, 1, 512, heads * DK), lambda i: (0, seq, 0, i))
    out = pl.BlockSpec((512, heads * DK), lambda i: (0, i))
    return pl.pallas_call(
        functools.partial(attention_kernel, heads),
        grid=(steps,),
        in_specs=[spec] * 4,
        out_specs=[out] * 2,
        out_shape=[jax.ShapeDtypeStruct((512, hidden), BF16)] * 2,
        compiler_params=pltpu.CompilerParams(vmem_limit_bytes=40 * GIB),
        cost_estimate=pl.CostEstimate(flops=4 * 10**9, bytes_accessed=6 * GIB, transcendentals=2 * GIB),
        name="attention",
    )(q, k, v, g)


def project_kernel(core_ref, kg_ref, vg_ref, wk_ref, wv_ref, out_ref):
    hidden = kg_ref.shape[1]
    wk = jnp.concatenate([wk_ref[0, :, zl, 0].reshape(256, hidden) for zl in range(2)], 0)
    wv = jnp.concatenate([wv_ref[0, :, zl, 0].reshape(256, hidden) for zl in range(2)], 0)
    out_ref[...] = dot(wk, kg_ref[...], NT) + dot(wv, vg_ref[...], NT)


def project(core, kg, vg, wk, wv):
    hidden = kg.shape[1]
    weight = pl.BlockSpec((1, 4, 2, 1, 64, hidden), lambda i, core: (0, 0, 0, core[0], 0, 0))
    whole = pl.BlockSpec((512, hidden), lambda i, core: (0, 0))
    return pl.pallas_call(
        project_kernel,
        grid_spec=pltpu.PrefetchScalarGridSpec(
            num_scalar_prefetch=1,
            grid=(1,),
            in_specs=[whole, whole, weight, weight],
            out_specs=pl.BlockSpec((512, 512), lambda i, core: (0, 0)),
        ),
        out_shape=jax.ShapeDtypeStruct((512, 512), F32),
        compiler_params=pltpu.CompilerParams(vmem_limit_bytes=40 * GIB),
        cost_estimate=pl.CostEstimate(flops=10**9, bytes_accessed=5 * GIB, transcendentals=0),
        name="project",
    )(core.reshape(1), kg, vg, wk, wv)


def small(kernel, outs, name, n_scalar, *args):
    specs = [SMEM] * n_scalar + [VMEM] * (len(args) - n_scalar)
    return pl.pallas_call(
        kernel,
        in_specs=specs,
        out_specs=[VMEM] * len(outs),
        out_shape=[jax.ShapeDtypeStruct(s, F32) for s in outs],
        compiler_params=pltpu.CompilerParams(vmem_limit_bytes=24 * GIB),
        cost_estimate=pl.CostEstimate(flops=10**6, bytes_accessed=GIB, transcendentals=0),
        name=name,
    )(*args)


X_SHIFTS = (2, 1, 3, 0)


def pair_kernel(x_ref, own_ref, got_ref, *out_refs):
    for shift, out_ref in zip(X_SHIFTS, out_refs):
        owner = lax.rem(x_ref[0] + shift, 4)
        lanes = pl.ds(pl.multiple_of(owner * 128, 128), 128)
        out_ref[...] = own_ref[:, lanes] + got_ref[:, lanes]


MIXES = ((1, 1), (1, 0), (0, 1), (0, 0))


def mix_kernel(yh_ref, zl_ref, *refs):
    ins, outs, scratch = refs[:8], refs[8:12], refs[12]
    first = (ins[0][...] + ins[1][...]) + (ins[2][...] + ins[3][...])
    second = (ins[4][...] + ins[5][...]) + (ins[6][...] + ins[7][...])
    low = lax.broadcasted_iota(jnp.int32, first.shape, 1) < 64
    scratch[0] = jnp.where(low, first, pltpu.roll(second, 64, 1))
    scratch[1] = jnp.where(low, pltpu.roll(first, 64, 1), second)
    for (dy, dz), out_ref in zip(MIXES, outs):
        yh = lax.rem(yh_ref[0] + dy, 2)
        zl = lax.rem(zl_ref[0] + dz, 2)
        out_ref[...] = scratch[yh, pl.ds(pl.multiple_of(zl * 256, 256), 256), :]


Z_SHIFTS = (2, 1, 3, 0)


def spread_kernel(zh_ref, *refs):
    parts, gains, squares_ref, outs, gathered = refs[:4], refs[4:8], refs[8], refs[9:13], refs[13]
    for shift, ref in zip(Z_SHIFTS, gains):
        gathered[lax.rem(zh_ref[0] + 4 - shift, 4)] = ref[...]
    total = (parts[0][...] + parts[1][...]) + (parts[2][...] + parts[3][...])
    weighted = gathered[...].reshape(256, 128)
    cross = jnp.sum(total * weighted, axis=0, keepdims=True)
    row = lax.broadcasted_iota(jnp.int32, (8, 128), 0)
    extra = jnp.where(row == 0, cross, jnp.where(row == 1, squares_ref[0:1, :], 0.0))
    blocks = total.reshape(4, 64, 128)
    for i in range(4):
        gathered[i] = blocks[i]
    for shift, out_ref in zip(Z_SHIFTS, outs):
        out_ref[0:64, :] = gathered[lax.rem(zh_ref[0] + shift, 4)]
        out_ref[64:72, :] = extra


def close_kernel(*refs):
    parts, grad_ref, extra_ref = refs[:4], refs[4], refs[5]
    total = (parts[0][...] + parts[1][...]) + (parts[2][...] + parts[3][...])
    grad_ref[...] = total[0:64]
    extra_ref[...] = total[64:72]


def finish_kernel(grad_ref, hidden_ref, gain_ref, a_ref, b_ref, c_ref, d_ref, out_ref):
    totals = (a_ref[...] + b_ref[...]) + (c_ref[...] + d_ref[...])
    cross, square = totals[0:1], totals[1:2]
    inverse = lax.rsqrt(square / D + epsilon)
    result = gain_ref[...] * grad_ref[...] * inverse - hidden_ref[...] * (
        cross * inverse * inverse * inverse / D
    )
    out_ref[...] = result.T


def open_kernel(hidden_ref, gain_ref, hidden_out, gain_out, weighted_out, squares_out):
    hidden = hidden_ref[...].T
    gain = jnp.broadcast_to(gain_ref[...], (128, 64)).T
    hidden_out[...] = hidden
    gain_out[...] = gain
    weighted_out[...] = hidden * gain
    squares_out[...] = jnp.broadcast_to(jnp.sum(hidden * hidden, axis=0, keepdims=True), (8, 128))


def shifted_by(array, axis, shift):
    n = lax.axis_size(axis)
    return lax.ppermute(array, axis, [(i, (i + shift) % n) for i in range(n)])


def mixed_by(array, axes, flips):
    pairs = []
    for a in range(2):
        for b in range(2):
            pairs.append((a * 2 + b, (a ^ flips[0]) * 2 + (b ^ flips[1])))
    return lax.ppermute(array, axes, pairs)


def per_device(q, k, v, g, wk, wv, hidden, gain):
    at = {name: lax.axis_index(name).astype(jnp.int32) for name in ("yh", "x", "zh", "zl", "c")}
    one = lambda name: at[name].reshape(1)
    features = wk.shape[2]
    wk = wk.reshape(1, 4, 2, 2, 64, features)
    wv = wv.reshape(1, 4, 2, 2, 64, features)

    hidden_t, gain_t, weighted, squares = small(
        open_kernel, [(64, 128)] * 3 + [(8, 128)], "open", 0, hidden.reshape(128, 64), gain.reshape(1, 64)
    )
    gathered = [shifted_by(weighted, "zh", s) for s in Z_SHIFTS[:3]] + [weighted]

    sums = []
    for seq in range(2):
        kg, vg = attention(seq, q, k, v, g)
        theirs = project(1 - at["c"], kg, vg, wk, wv)
        got = shifted_by(theirs, "c", 1)
        mine = project(at["c"], kg, vg, wk, wv)
        blocks = small(pair_kernel, [(512, 128)] * 4, "pair", 1, one("x"), mine, got)
        sums += [shifted_by(b, "x", s) for b, s in zip(blocks, X_SHIFTS[:3])] + [blocks[3]]

    mixed = pl.pallas_call(
        mix_kernel,
        in_specs=[SMEM] * 2 + [VMEM] * 8,
        out_specs=[VMEM] * 4,
        out_shape=[jax.ShapeDtypeStruct((256, 128), F32)] * 4,
        scratch_shapes=[pltpu.VMEM((2, 512, 128), F32)],
        cost_estimate=pl.CostEstimate(flops=10**6, bytes_accessed=GIB, transcendentals=0),
        name="mix",
    )(one("yh"), one("zl"), *sums)
    parts = [mixed_by(m, ("yh", "zl"), f) for m, f in zip(mixed, MIXES[:3])] + [mixed[3]]

    spread = pl.pallas_call(
        spread_kernel,
        in_specs=[SMEM] + [VMEM] * 9,
        out_specs=[VMEM] * 4,
        out_shape=[jax.ShapeDtypeStruct((72, 128), F32)] * 4,
        scratch_shapes=[pltpu.VMEM((4, 64, 128), F32)],
        cost_estimate=pl.CostEstimate(flops=10**6, bytes_accessed=GIB, transcendentals=0),
        name="spread",
    )(one("zh"), *parts, *gathered, squares)
    ends = [shifted_by(b, "zh", s) for b, s in zip(spread, Z_SHIFTS[:3])] + [spread[3]]
    grad, extra = small(close_kernel, [(64, 128), (8, 128)], "close", 0, *ends)
    extras = [mixed_by(extra, ("zl", "c"), f) for f in MIXES[:3]]
    (out,) = small(finish_kernel, [(128, 64)], "finish", 0, grad, hidden_t, gain_t, extra, *extras)
    return out.reshape(2, 64, 64)


def solution(mesh):
    section, tensor = ("yh", "x"), ("zh", "zl", "c")
    fine = Mesh(mesh.devices.reshape(2, 4, 4, 2, 2, 2), ("yh", "x", "zh", "zl", "c", "dp"))
    spread = P(section, "dp", None, tensor)
    return jax.shard_map(
        per_device,
        mesh=fine,
        in_specs=(
            spread,
            spread,
            spread,
            spread,
            P(section, None, tensor),
            P(section, None, tensor),
            P("dp", section, tensor),
            P(tensor),
        ),
        out_specs=P("dp", section, tensor),
        check_vma=False,
    )
```

```python
import functools

import jax
import jax.numpy as jnp
from jax import lax
from jax.experimental import pallas as pl
from jax.experimental.pallas import tpu as pltpu
from jax.sharding import Mesh, PartitionSpec as P


D = 1024
DK = 128
epsilon = 1e-06
F32 = jnp.float32
BF16 = jnp.bfloat16
VMEM = pl.BlockSpec(memory_space=pltpu.VMEM)
NT = (((1,), (1,)), ((), ()))
NN = (((1,), (0,)), ((), ()))
GIB = 2**20


def dot(a, b, dims):
    return lax.dot_general(a, b, dims, preferred_element_type=F32)


def by_owner(rows):
    return rows.reshape(2, 4, 64, DK).swapaxes(0, 1).reshape(512, DK)


WIDTH = 128


def attention_kernel(heads, q_ref, k_ref, v_ref, g_ref, *rest):
    kg_ref, vg_ref = rest[-2:]
    pieces = [(h, p) for h in range(heads) for p in range(512 // WIDTH)]
    sums = {}

    def queries(h, p):
        rows, cols = pl.ds(p * WIDTH, WIDTH), pl.ds(h * DK, DK)
        return q_ref[0, 0, rows, cols], g_ref[0, 0, rows, cols]

    def first(h, p):
        q, g = queries(h, p)
        cols = pl.ds(h * DK, DK)
        k, v = by_owner(k_ref[0, 0, :, cols]), by_owner(v_ref[0, 0, :, cols])
        return dot(k, q, NT), dot(v, g, NT)

    def middle(scores, prob_grad):
        shifted = jnp.exp(scores - jnp.max(scores, axis=0, keepdims=True))
        inverse = 1.0 / jnp.sum(shifted, axis=0, keepdims=True)
        row_dot = jnp.sum(shifted * prob_grad, axis=0, keepdims=True) * inverse
        probs = shifted * inverse
        return probs.astype(BF16), (probs * (prob_grad - row_dot)).astype(BF16)

    def last(h, p, low, score_low):
        q, g = queries(h, p)
        kg, vg = dot(score_low, q, NN), dot(low, g, NN)
        sums[h] = (kg, vg) if p == 0 else (sums[h][0] + kg, sums[h][1] + vg)
        if p == 512 // WIDTH - 1:
            cols = pl.ds(h * DK, DK)
            kg_ref[:, cols] = sums[h][0].astype(BF16)
            vg_ref[:, cols] = sums[h][1].astype(BF16)

    ahead, before = first(*pieces[0]), None
    for i, piece in enumerate(pieces):
        now, ahead = ahead, first(*pieces[i + 1]) if i + 1 < len(pieces) else None
        low = middle(*now)
        if before is not None:
            last(*before)
        before = (*piece, *low)
    last(*before)


ANY = pl.BlockSpec(memory_space=pl.ANY)


def attention(seq, q, k, v, g, after, heads=4):
    hidden = q.shape[3]
    steps = hidden // (heads * DK)
    spec = pl.BlockSpec((1, 1, 512, heads * DK), lambda i: (0, seq, 0, i))
    out = pl.BlockSpec((512, heads * DK), lambda i: (0, i))
    return pl.pallas_call(
        functools.partial(attention_kernel, heads),
        grid=(steps,),
        in_specs=[spec] * 4 + [ANY] * len(after),
        out_specs=[out] * 2,
        out_shape=[jax.ShapeDtypeStruct((512, hidden), BF16)] * 2,
        compiler_params=pltpu.CompilerParams(vmem_limit_bytes=20 * GIB),
        cost_estimate=pl.CostEstimate(flops=4 * 10**9, bytes_accessed=6 * GIB, transcendentals=2 * GIB),
        name="attention",
    )(q, k, v, g, *after)


def project_kernel(other, kg_ref, vg_ref, wk_ref, wv_ref, out_ref):
    hidden = kg_ref.shape[1]
    core = lax.axis_index("c")
    core = 1 - core if other else core
    wk = jnp.concatenate([wk_ref[0, :, zl, core].reshape(256, hidden) for zl in range(2)], 0)
    wv = jnp.concatenate([wv_ref[0, :, zl, core].reshape(256, hidden) for zl in range(2)], 0)
    out_ref[...] = dot(wk, kg_ref[...], NT) + dot(wv, vg_ref[...], NT)


def project(other, kg, vg, wk, wv):
    return pl.pallas_call(
        functools.partial(project_kernel, other),
        in_specs=[VMEM] * 4,
        out_specs=VMEM,
        out_shape=jax.ShapeDtypeStruct((512, 512), F32),
        compiler_params=pltpu.CompilerParams(vmem_limit_bytes=8 * GIB),
        cost_estimate=pl.CostEstimate(flops=10**9, bytes_accessed=5 * GIB, transcendentals=0),
        name="project",
    )(kg, vg, wk, wv)


def small(kernel, outs, *args, after=(), scratch=()):
    specs = [VMEM] * len(args) + [ANY] * len(after)
    return pl.pallas_call(
        kernel,
        in_specs=specs,
        out_specs=[VMEM] * len(outs),
        out_shape=[jax.ShapeDtypeStruct(s, F32) for s in outs],
        scratch_shapes=[pltpu.VMEM(s, F32) for s in scratch],
        compiler_params=pltpu.CompilerParams(vmem_limit_bytes=8 * GIB),
        cost_estimate=pl.CostEstimate(flops=10**6, bytes_accessed=GIB, transcendentals=0),
    )(*args, *after)


X_SHIFTS = (2, 1, 3, 0)


def block_of(ref, owner, rows=slice(None)):
    return ref[rows, pl.ds(pl.multiple_of(owner * 128, 128), 128)]


def pair_kernel(own_ref, got_ref, *out_refs):
    for shift, out_ref in zip(X_SHIFTS, out_refs):
        owner = lax.rem(lax.axis_index("x") + shift, 4)
        out_ref[...] = block_of(own_ref, owner) + block_of(got_ref, owner)


def halves_kernel(own_ref, got_ref, *out_refs):
    x = lax.axis_index("x")
    for half, flips in enumerate(((1, 2, 0, 3), (3, 2, 0, 1))):
        rows = pl.ds(half * 256, 256)
        for i, flip in enumerate(flips):
            owner = lax.bitwise_xor(x, flip)
            out_ref = out_refs[half * 2 + i // 2]
            lanes = pl.ds((i % 2) * 128, 128)
            out_ref[:, lanes] = block_of(own_ref, owner, rows) + block_of(got_ref, owner, rows)


def fold_kernel(keep_a, got_a, keep_b, got_b, *refs):
    mine_a, send_a, mine_b, send_b = refs[-4:]
    for keep, got, mine, send in ((keep_a, got_a, mine_a, send_a), (keep_b, got_b, mine_b, send_b)):
        mine[...] = keep[:, 0:128] + got[:, 0:128]
        send[...] = keep[:, 128:256] + got[:, 128:256]


MIXES = ((1, 1), (1, 0), (0, 1), (0, 0))


def mix_kernel(*refs):
    ins, outs, scratch = refs[:8], refs[-5:-1], refs[-1]
    first = jnp.concatenate([ins[0][...] + ins[1][...], ins[2][...] + ins[3][...]], 0)
    second = (ins[4][...] + ins[5][...]) + (ins[6][...] + ins[7][...])
    low = lax.broadcasted_iota(jnp.int32, first.shape, 1) < 64
    scratch[0] = jnp.where(low, first, pltpu.roll(second, 64, 1))
    scratch[1] = jnp.where(low, pltpu.roll(first, 64, 1), second)
    for (dy, dz), out_ref in zip(MIXES, outs):
        yh = lax.rem(lax.axis_index("yh") + dy, 2)
        zl = lax.rem(lax.axis_index("zl") + dz, 2)
        out_ref[...] = scratch[yh, pl.ds(pl.multiple_of(zl * 256, 256), 256), :]


Z_SHIFTS = (2, 1, 3, 0)


def grow_kernel(own_ref, got_ref, *refs):
    refs[-1][0:64] = own_ref[...]
    refs[-1][64:128] = got_ref[...]


def spread_kernel(*refs):
    parts, near_ref, far_ref, squares_ref = refs[:4], refs[4], refs[5], refs[6]
    outs, gathered = refs[-5:-1], refs[-1]
    zh = lax.axis_index("zh")
    for flip, ref, row in ((0, near_ref, 0), (1, near_ref, 64), (2, far_ref, 0), (3, far_ref, 64)):
        gathered[lax.bitwise_xor(zh, flip)] = ref[row : row + 64]
    total = (parts[0][...] + parts[1][...]) + (parts[2][...] + parts[3][...])
    weighted = gathered[...].reshape(256, 128)
    cross = jnp.sum(total * weighted, axis=0, keepdims=True)
    row = lax.broadcasted_iota(jnp.int32, (8, 128), 0)
    extra = jnp.where(row == 0, cross, jnp.where(row == 1, squares_ref[0:1, :], 0.0))
    blocks = total.reshape(4, 64, 128)
    for i in range(4):
        gathered[i] = blocks[i]
    for shift, out_ref in zip(Z_SHIFTS, outs):
        out_ref[0:64, :] = gathered[lax.rem(zh + shift, 4)]
        out_ref[64:72, :] = extra


def close_kernel(*refs):
    parts, grad_ref, extra_ref = refs[:4], refs[4], refs[5]
    total = (parts[0][...] + parts[1][...]) + (parts[2][...] + parts[3][...])
    grad_ref[...] = total[0:64]
    extra_ref[...] = total[64:72]


def finish_kernel(grad_ref, hidden_ref, gain_ref, a_ref, b_ref, c_ref, d_ref, out_ref):
    totals = (a_ref[...] + b_ref[...]) + (c_ref[...] + d_ref[...])
    cross, square = totals[0:1], totals[1:2]
    inverse = lax.rsqrt(square / D + epsilon)
    result = gain_ref[...] * grad_ref[...] * inverse - hidden_ref[...] * (
        cross * inverse * inverse * inverse / D
    )
    out_ref[...] = result.T


def open_kernel(hidden_ref, gain_ref, *refs):
    hidden_out, gain_out, weighted_out, squares_out = refs[-4:]
    hidden = hidden_ref[...].T
    gain = jnp.broadcast_to(gain_ref[...], (128, 64)).T
    hidden_out[...] = hidden
    gain_out[...] = gain
    weighted_out[...] = hidden * gain
    squares_out[...] = jnp.broadcast_to(jnp.sum(hidden * hidden, axis=0, keepdims=True), (8, 128))


def shifted_by(array, axis, shift):
    n = lax.axis_size(axis)
    return lax.ppermute(array, axis, [(i, (i + shift) % n) for i in range(n)])


def flipped_by(array, axis, flip):
    return lax.ppermute(array, axis, [(i, i ^ flip) for i in range(lax.axis_size(axis))])


def mixed_by(array, axes, flips):
    pairs = []
    for a in range(2):
        for b in range(2):
            pairs.append((a * 2 + b, (a ^ flips[0]) * 2 + (b ^ flips[1])))
    return lax.ppermute(array, axes, pairs)


def per_device(q, k, v, g, wk, wv, hidden, gain):
    features = wk.shape[2]
    wk = wk.reshape(1, 4, 2, 2, 64, features)
    wv = wv.reshape(1, 4, 2, 2, 64, features)

    q, k, v, g = (pltpu.with_memory_space_constraint(x, pltpu.HBM) for x in (q, k, v, g))

    kg, vg = attention(0, q, k, v, g, ())
    theirs = project(True, kg, vg, wk, wv)
    got = flipped_by(theirs, "c", 1)
    mine = project(False, kg, vg, wk, wv)
    hidden_t, gain_t, weighted, squares = small(
        open_kernel,
        [(64, 128)] * 3 + [(8, 128)],
        hidden.reshape(128, 64),
        gain.reshape(1, 64),
        after=(mine,),
    )
    near = flipped_by(weighted, "zh", 1)
    send_a, keep_a, send_b, keep_b = small(halves_kernel, [(256, 256)] * 4, mine, got)
    got_a = flipped_by(send_a, "x", 1)
    got_b = flipped_by(send_b, "x", 3)

    kg, vg = attention(1, q, k, v, g, (keep_a,))
    theirs = project(True, kg, vg, wk, wv)
    got = flipped_by(theirs, "c", 1)
    mine = project(False, kg, vg, wk, wv)
    mine_a, send_a, mine_b, send_b = small(
        fold_kernel, [(256, 128)] * 4, keep_a, got_a, keep_b, got_b, after=(mine,)
    )
    got_a = flipped_by(send_a, "x", 3)
    got_b = flipped_by(send_b, "x", 1)
    blocks = small(pair_kernel, [(512, 128)] * 4, mine, got)
    direct = []
    for block, shift in zip(blocks, X_SHIFTS[:3]):
        direct.append(shifted_by(block, "x", shift))
    grown = small(grow_kernel, [(128, 128)], weighted, near, after=(blocks[3],))[0]
    far = flipped_by(grown, "zh", 2)

    mixed = small(
        mix_kernel,
        [(256, 128)] * 4,
        mine_a,
        got_a,
        mine_b,
        got_b,
        *direct,
        blocks[3],
        scratch=[(2, 512, 128)],
    )
    parts = [mixed_by(m, ("yh", "zl"), f) for m, f in zip(mixed, MIXES[:3])] + [mixed[3]]

    spread = small(
        spread_kernel, [(72, 128)] * 4, *parts, grown, far, squares, scratch=[(4, 64, 128)]
    )
    ends = [shifted_by(b, "zh", s) for b, s in zip(spread, Z_SHIFTS[:3])] + [spread[3]]
    grad, extra = small(close_kernel, [(64, 128), (8, 128)], *ends)
    extras = [mixed_by(extra, ("zl", "c"), f) for f in MIXES[:3]]
    (out,) = small(finish_kernel, [(128, 64)], grad, hidden_t, gain_t, extra, *extras)
    return out.reshape(2, 64, 64)


def solution(mesh):
    section, tensor = ("yh", "x"), ("zh", "zl", "c")
    fine = Mesh(mesh.devices.reshape(2, 4, 4, 2, 2, 2), ("yh", "x", "zh", "zl", "c", "dp"))
    spread = P(section, "dp", None, tensor)
    return jax.shard_map(
        per_device,
        mesh=fine,
        in_specs=(
            spread,
            spread,
            spread,
            spread,
            P(section, None, tensor),
            P(section, None, tensor),
            P("dp", section, tensor),
            P(tensor),
        ),
        out_specs=P("dp", section, tensor),
        check_vma=False,
    )
```
